32 devices in a mesh: section: 2 (over x), tensor: 8 (over z, core), dp: 2 (over y).
Axes of the slice: x: 2, y: 2, z: 4, core: 2. Of those that a mesh axis runs over, the one named last changes fastest.
Arguments:
- dec_queries: bfloat16 [2, 4, 512, 8192], P('section', 'dp', None, 'tensor'), may hold values from -8 to 8
- enc_keys: bfloat16 [2, 4, 512, 8192], P('section', 'dp', None, 'tensor'), may hold values from -4 to 4
- enc_values: bfloat16 [2, 4, 512, 8192], P('section', 'dp', None, 'tensor'), may hold values from -4 to 4
- out_grad: bfloat16 [2, 4, 512, 8192], P('section', 'dp', None, 'tensor'), may hold values from -15 to 15
- key_weight: bfloat16 [2, 1024, 8192], P('section', None, 'tensor'), may hold values from -0.1875 to 0.1875
- value_weight: bfloat16 [2, 1024, 8192], P('section', None, 'tensor'), may hold values from -0.1875 to 0.1875
- enc_hidden: float32 [4, 512, 1024], P('dp', 'section', 'tensor'), may hold values from -2 to 2, as said below
- enc_gain: float32 [1024], P('tensor'), may hold values from 0.1 to 1.9
Outputs:
- enc_input_grad: float32 [4, 512, 1024], P('dp', 'section', 'tensor')
The draws below stay inside these ranges and needn't reach their ends.
Inputs may be any that keep to these rules, and one draw needn't show every extreme that they name: `enc_hidden`: every entry's magnitude is at least 0.25.
All inputs are finite; a program needn't handle non-finite values.
Results may differ from the reference program's by a relative error of at most 0.0041.
Values sent between devices are 32-bit elements; how exact they have to be, the bound alone decides.
A program may use at most 128 MiB of HBM per device.

```python
import jax
import jax.numpy as jnp
from jax import lax

D = 1024
DK = 128
DEC = 512
ENC = 512
HEADS = 64
INNER = 8192
SECTIONS = 2
SEQS = 4


def shared_rows(key):
    return jnp.clip(jax.random.normal(jax.random.fold_in(key, 12), (SECTIONS, SEQS, 1, INNER), jnp.float32), -4.0, 4.0)


def aligned_spot(key):
    return jax.random.randint(jax.random.fold_in(key, 13), (), 0, ENC).astype(jnp.int32)


def draw_enc_keys(key, part):
    base = jnp.clip(jax.random.normal(jax.random.fold_in(key, 11), (SECTIONS, SEQS, ENC, INNER), jnp.float32), -4.0, 4.0)
    zero = jnp.zeros((), jnp.int32)
    base = lax.dynamic_update_slice(base, shared_rows(key), (zero, zero, aligned_spot(key), zero))
    return base.astype(jnp.bfloat16)


def draw_dec_queries(key, part):
    base = 0.1 * jnp.clip(jax.random.normal(jax.random.fold_in(key, 22), (SECTIONS, SEQS, DEC, INNER), jnp.float32), -6.0, 6.0)
    return base.astype(jnp.bfloat16)


def draw_enc_hidden(key, part):
    shape = (SEQS, ENC, D)
    own_sign = jnp.where(jax.random.bernoulli(jax.random.fold_in(key, 31), 0.5, shape), 1.0, -1.0)
    magnitude = jax.random.uniform(jax.random.fold_in(key, 36), shape, jnp.float32, 0.25, 2.0)
    sign = own_sign
    return (sign * magnitude).astype(jnp.float32)


def levels(key, dims, cuts, smallest, high):
    factor_of, own = 1.0, jax.random.fold_in(key, 6)
    for position, parts in cuts:
        draws = jnp.exp(jax.random.uniform(jax.random.fold_in(own, position), (parts,), jnp.float32, smallest / len(cuts), high / len(cuts)))
        factor_of = factor_of * jnp.repeat(draws, dims[position] // parts).reshape([-1 if axis == position else 1 for axis in range(len(dims))])
    return factor_of


def normal_values(rng, extent, spread, most, shards=(), kind=jnp.bfloat16):
    values = jax.random.normal(rng, extent, jnp.float32) * spread
    if len(shards) > 0:
        values = levels(rng, extent, shards, -0.22, 0.18) * values
    return jnp.clip(values, min=-most, max=most).astype(kind)


def setup_inputs(seed: int = 0) -> dict:
    seeds = jax.random.split(jax.random.key(seed), 9)
    return {
        "dec_queries": draw_dec_queries(jax.random.fold_in(seeds[8], 71), 0),
        "enc_keys": draw_enc_keys(jax.random.fold_in(seeds[8], 71), 0),
        "enc_values": normal_values(seeds[2], (SECTIONS, SEQS, ENC, INNER), 1.0, 4.0, ((0, 2), (1, 2), (3, 8))),
        "out_grad": normal_values(seeds[3], (SECTIONS, SEQS, DEC, INNER), 3.0, 15.0, ((0, 2), (1, 2), (3, 8))),
        "key_weight": normal_values(seeds[4], (SECTIONS, D, INNER), D ** -0.5, 0.1875, ((0, 2), (2, 8))),
        "value_weight": normal_values(seeds[5], (SECTIONS, D, INNER), D ** -0.5, 0.1875, ((0, 2), (2, 8))),
        "enc_hidden": draw_enc_hidden(jax.random.fold_in(seeds[8], 71), 0),
        "enc_gain": jnp.clip(1.0 + 0.18 * jax.random.normal(seeds[7], (D,), jnp.float32), 0.1, 1.9),
    }


def attention_grads(query, keyset, valueset, gradset):
    query_heads = query.reshape(DEC, HEADS, DK).astype(jnp.float32)
    key_heads = keyset.reshape(ENC, HEADS, DK).astype(jnp.float32)
    value_heads = valueset.reshape(ENC, HEADS, DK).astype(jnp.float32)
    grad_heads = gradset.reshape(DEC, HEADS, DK).astype(jnp.float32)
    scores = jnp.einsum('qhd,khd->hqk', query_heads, key_heads)
    shifted = jnp.exp(scores - lax.optimization_barrier(jnp.max(scores, axis=-1, keepdims=True)))
    attn_probs = shifted / lax.optimization_barrier(jnp.sum(shifted, axis=-1, keepdims=True))
    probs_low = lax.optimization_barrier(attn_probs.astype(jnp.bfloat16)).astype(jnp.float32)
    attended = jnp.einsum('hqk,khd->qhd', probs_low, value_heads)
    row_dot = lax.optimization_barrier(jnp.sum(grad_heads * attended, axis=-1))
    value_grad = jnp.einsum('hqk,qhd->khd', probs_low, grad_heads).astype(jnp.bfloat16)
    prob_grad = jnp.einsum('qhd,khd->hqk', grad_heads, value_heads)
    score_grad = attn_probs * (prob_grad - jnp.transpose(row_dot)[:, :, None])
    score_low = lax.optimization_barrier(score_grad.astype(jnp.bfloat16)).astype(jnp.float32)
    key_grad = jnp.einsum('hqk,qhd->khd', score_low, query_heads).astype(jnp.bfloat16)
    return (key_grad.reshape(ENC, HEADS * DK), value_grad.reshape(ENC, HEADS * DK))

def reference(dec_queries, enc_keys, enc_values, out_grad, key_weight, value_weight, enc_hidden, enc_gain):

    def section_term(pieces):
        query, keyset, valueset, gradset, weight_k, weight_v = pieces

        def seq_term(inner):
            key_grad, value_grad = attention_grads(inner[0], inner[1], inner[2], inner[3])
            first = jnp.dot(key_grad, jnp.transpose(weight_k), preferred_element_type=jnp.float32)
            second = jnp.dot(value_grad, jnp.transpose(weight_v), preferred_element_type=jnp.float32)
            return first + second
        return lax.map(seq_term, (query, keyset, valueset, gradset))
    terms = lax.map(section_term, (dec_queries, enc_keys, enc_values, out_grad, key_weight, value_weight))
    enc_grad = lax.optimization_barrier(jnp.sum(terms, axis=0))
    scaled = enc_gain * enc_grad
    square_total = lax.optimization_barrier(jnp.sum(enc_hidden * enc_hidden, axis=-1))
    cross_total = lax.optimization_barrier(jnp.sum(scaled * enc_hidden, axis=-1))
    inverse = lax.rsqrt(square_total / D + 1e-06)
    return scaled * inverse[..., None] - enc_hidden * (cross_total * inverse * inverse * inverse / D)[..., None]
```

```python
import functools

import jax
import jax.numpy as jnp
from jax import lax
from jax.experimental import pallas as pl
from jax.experimental.pallas import tpu as pltpu
from jax.sharding import PartitionSpec as P

DK = 128
CORES = 2
EPSILON = 1e-06
MESH = pl.DeviceIdType.MESH
F32 = jnp.float32
BF16 = jnp.bfloat16
QUERY_BLOCK = 256


def dot_nt(a, b, precision=None):
    return lax.dot_general(
        a, b, (((1,), (1,)), ((), ())), precision=precision, preferred_element_type=F32
    )


def dot_nn(a, b):
    return lax.dot_general(a, b, (((1,), (0,)), ((), ())), preferred_element_type=F32)


def dot_tn(a, b, precision=None):
    return lax.dot_general(
        a, b, (((0,), (0,)), ((), ())), precision=precision, preferred_element_type=F32
    )


def body(
    sections, tensors, query_block,
    q_hbm, k_hbm, v_hbm, g_hbm, wk_hbm, wv_hbm, hidden_hbm, gain_hbm,
    out_ref,
    q_buf, k_buf, v_buf, g_buf, w_buf, hidden, gain, grads,
    part, pair_in, section_in, line_out, line_in,
    square_out, square_in, cross_out, cross_in,
    load_sem, weight_sem, small_sem,
    pair_send, pair_recv, section_send, section_recv, line_send, line_recv,
    square_send, square_recv, cross_send, cross_recv,
):
    seqs, heads, dec_len, _ = q_buf.shape
    enc_len = k_buf.shape[2]
    inner = heads * DK
    model_width = w_buf.shape[0]
    feats = out_ref.shape[2]
    rows = out_ref.shape[1]
    chips = tensors // CORES
    s_me = lax.axis_index("section")
    t_me = lax.axis_index("tensor")
    z_me = lax.div(t_me, CORES)
    c_me = lax.rem(t_me, CORES)
    partner = z_me * CORES + (CORES - 1 - c_me)

    def loads(b, h):
        cols = pl.ds(pl.multiple_of(h * DK, DK), DK)
        return [
            pltpu.make_async_copy(src.at[0, b, :, cols], dst.at[b, h], load_sem.at[i, b, h])
            for i, (src, dst) in enumerate(
                ((q_hbm, q_buf), (k_hbm, k_buf), (v_hbm, v_buf), (g_hbm, g_buf))
            )
        ]

    def start_loads(b):
        def step(h, carry):
            for copy in loads(b, h):
                copy.start()
            return carry

        lax.fori_loop(0, heads, step, 0)

    weight_copies = [
        pltpu.make_async_copy(src.at[0], w_buf.at[:, pl.ds(i * inner, inner)], weight_sem.at[i])
        for i, src in enumerate((wk_hbm, wv_hbm))
    ]
    small_copies = [
        pltpu.make_async_copy(hidden_hbm, hidden, small_sem.at[0]),
        pltpu.make_async_copy(gain_hbm, gain, small_sem.at[1]),
    ]

    start_loads(0)
    for copy in small_copies + weight_copies:
        copy.start()
    for b in range(1, seqs):
        start_loads(b)

    barrier = pltpu.get_barrier_semaphore()
    for i in range(1, tensors):
        pl.semaphore_signal(
            barrier, inc=1, device_id={"tensor": lax.rem(t_me + i, tensors)}, device_id_type=MESH
        )
    for i in range(1, sections):
        pl.semaphore_signal(
            barrier, inc=1, device_id={"section": lax.rem(s_me + i, sections)}, device_id_type=MESH
        )

    def head(b, h):
        for copy in loads(b, h):
            copy.wait()
        keys = k_buf[b, h]
        values = v_buf[b, h]
        key_grad = None
        for start in range(0, dec_len, query_block):
            queries = q_buf[b, h, pl.ds(start, query_block), :]
            out_grads = g_buf[b, h, pl.ds(start, query_block), :]
            scores = dot_nt(keys, queries)
            shifted = jnp.exp(scores - jnp.max(scores, axis=0, keepdims=True))
            probs = shifted * (1.0 / jnp.sum(shifted, axis=0, keepdims=True))
            probs_low = probs.astype(BF16)
            prob_grad = dot_nt(values, out_grads)
            row_dot = jnp.sum(probs_low.astype(F32) * prob_grad, axis=0, keepdims=True)
            score_low = (probs * (prob_grad - row_dot)).astype(BF16)
            value_term = dot_nn(probs_low, out_grads)
            key_term = dot_nn(score_low, queries)
            if key_grad is None:
                key_grad, value_grad = key_term, value_term
            else:
                key_grad, value_grad = key_grad + key_term, value_grad + value_term
        grads[:, pl.ds(pl.multiple_of(h * DK, DK), DK)] = key_grad.astype(BF16)
        grads[:, pl.ds(pl.multiple_of(inner + h * DK, DK), DK)] = value_grad.astype(BF16)

    def pair_copy(b, k):
        return pltpu.make_async_remote_copy(
            src_ref=part.at[b, k, CORES - 1 - c_me], dst_ref=pair_in.at[b, k],
            send_sem=pair_send.at[b, k], recv_sem=pair_recv.at[b, k],
            device_id={"tensor": partner}, device_id_type=MESH,
        )

    def section_copies(b, k):
        copies = []
        for i in range(1, sections):
            target = lax.rem(s_me + i, sections)
            copies.append(pltpu.make_async_remote_copy(
                src_ref=part.at[b, k, c_me, target], dst_ref=section_in.at[b, k, i - 1],
                send_sem=section_send.at[b, k, i - 1], recv_sem=section_recv.at[b, k, i - 1],
                device_id={"section": target}, device_id_type=MESH,
            ))
        return copies

    def line_copy(b, k):
        target = lax.rem(z_me + 1 + k, chips) * CORES + c_me
        return pltpu.make_async_remote_copy(
            src_ref=line_out.at[b, k], dst_ref=line_in.at[b, k],
            send_sem=line_send.at[b, k], recv_sem=line_recv.at[b, k],
            device_id={"tensor": target}, device_id_type=MESH,
        )

    def stat_copies(src, dst, send, recv):
        return [
            pltpu.make_async_remote_copy(
                src_ref=src, dst_ref=dst.at[i - 1],
                send_sem=send.at[i - 1], recv_sem=recv.at[i - 1],
                device_id={"tensor": lax.rem(t_me + i, tensors)}, device_id_type=MESH,
            )
            for i in range(1, tensors)
        ]

    def square_copies():
        return stat_copies(square_out, square_in, square_send, square_recv)

    def cross_copies(b):
        return stat_copies(
            cross_out.at[b], cross_in.at[b], cross_send.at[b], cross_recv.at[b]
        )

    def lane_sums(x):
        total = dot_nt(jnp.ones((8, feats), F32), x, lax.Precision.HIGHEST)
        return total[0:1, :]

    def spread(row):
        return dot_tn(
            jnp.broadcast_to(row, (8, rows)), jnp.full((8, feats), 0.125, F32),
            lax.Precision.HIGHEST,
        )

    def project(b, k):
        chip = lax.rem(z_me + 1 + k, chips)
        width = CORES * feats
        block = dot_nt(
            grads[...], w_buf[pl.ds(pl.multiple_of(chip * width, width), width), :]
        )
        for half in range(CORES):
            part[b, k, half] = block[:, half * feats : (half + 1) * feats].reshape(
                sections, rows, feats
            )
        pair_copy(b, k).start()

    def pair_step(b, k):
        pair_copy(b, k).wait_recv()
        part[b, k, c_me] = part[b, k, c_me] + pair_in[b, k]
        for copy in section_copies(b, k):
            copy.start()

    def section_step(b, k):
        total = part[b, k, c_me, s_me]
        for i, copy in enumerate(section_copies(b, k)):
            copy.wait_recv()
            total = total + section_in[b, k, i]
        line_out[b, k] = total

    def loop(low, high, step):
        def run(i, carry):
            step(i)
            return carry

        lax.fori_loop(low, high, run, 0)

    def forward(b, k):
        section_step(b, k)
        line_copy(b, k).start()

    def finish_sum(b):
        section_step(b, chips - 1)
        total = line_out[b, chips - 1]
        for k in range(chips - 1):
            line_copy(b, k).wait_recv()
            total = total + line_in[b, k]
        scaled = gain[...] * total
        out_ref[b] = scaled
        cross_out[b] = lane_sums(scaled * hidden[b])
        for copy in cross_copies(b):
            copy.start()

    def finish_norm(b):
        for copy in cross_copies(b):
            copy.wait_recv()
        cross = cross_out[b]
        square = square_out[b]
        for i in range(tensors - 1):
            cross = cross + cross_in[b, i]
            square = square + square_in[i, b]
        inverse = lax.rsqrt(square / model_width + EPSILON)
        factor = cross * inverse * inverse * inverse / model_width
        out_ref[b] = out_ref[b] * spread(inverse) - hidden[b] * spread(factor)

    heads_per_step = heads // chips
    for b in range(seqs):
        def heads_step(k):
            loop(0, heads_per_step, lambda i: head(b, k * heads_per_step + i))
            if b > 0:
                @pl.when(k < chips - 1)
                def _():
                    forward(b - 1, k)

        if b == 0:
            loop(0, heads, lambda h: head(b, h))
            for copy in small_copies:
                copy.wait()
            for i in range(seqs):
                square_out[i] = lane_sums(hidden[i] * hidden[i])
            for copy in weight_copies:
                copy.wait()
            pl.semaphore_wait(barrier, tensors - 1 + sections - 1)
            for copy in square_copies():
                copy.start()
        else:
            loop(0, chips, heads_step)

        project(b, 0)

        def project_step(k):
            project(b, k)
            pair_step(b, k - 1)

        loop(1, chips, project_step)
        pair_step(b, chips - 1)

    for copy in square_copies():
        copy.wait_recv()
    for b in range(seqs - 1):
        finish_sum(b)
    loop(0, chips - 1, lambda k: forward(seqs - 1, k))
    finish_sum(seqs - 1)
    for b in range(seqs):
        finish_norm(b)

    for copy in square_copies():
        copy.wait_send()
    for b in range(seqs):
        for copy in cross_copies(b):
            copy.wait_send()

        def drain(k):
            pair_copy(b, k).wait_send()
            for copy in section_copies(b, k):
                copy.wait_send()

        loop(0, chips, drain)
        loop(0, chips - 1, lambda k: line_copy(b, k).wait_send())


def per_device(
    sections, tensors,
    dec_queries, enc_keys, enc_values, out_grad, key_weight, value_weight, enc_hidden, enc_gain,
):
    _, seqs, dec_len, inner = dec_queries.shape
    enc_len = enc_keys.shape[2]
    heads = inner // DK
    model_width = key_weight.shape[1]
    chips = tensors // CORES
    feats = model_width // tensors
    rows = enc_len // sections
    dma = pltpu.SemaphoreType.DMA
    call = pl.pallas_call(
        functools.partial(body, sections, tensors, min(QUERY_BLOCK, dec_len)),
        out_shape=jax.ShapeDtypeStruct((seqs, rows, feats), F32),
        in_specs=[pl.BlockSpec(memory_space=pl.ANY)] * 8,
        out_specs=pl.BlockSpec(memory_space=pltpu.VMEM),
        scratch_shapes=[
            pltpu.VMEM((seqs, heads, dec_len, DK), BF16),
            pltpu.VMEM((seqs, heads, enc_len, DK), BF16),
            pltpu.VMEM((seqs, heads, enc_len, DK), BF16),
            pltpu.VMEM((seqs, heads, dec_len, DK), BF16),
            pltpu.VMEM((model_width, 2 * inner), BF16),
            pltpu.VMEM((seqs, rows, feats), F32),
            pltpu.VMEM((1, feats), F32),
            pltpu.VMEM((enc_len, 2 * inner), BF16),
            pltpu.VMEM((seqs, chips, CORES, sections, rows, feats), F32),
            pltpu.VMEM((seqs, chips, sections, rows, feats), F32),
            pltpu.VMEM((seqs, chips, sections - 1, rows, feats), F32),
            pltpu.VMEM((seqs, chips, rows, feats), F32),
            pltpu.VMEM((seqs, chips - 1, rows, feats), F32),
            pltpu.VMEM((seqs, 1, rows), F32),
            pltpu.VMEM((tensors - 1, seqs, 1, rows), F32),
            pltpu.VMEM((seqs, 1, rows), F32),
            pltpu.VMEM((seqs, tensors - 1, 1, rows), F32),
            dma((4, seqs, heads)),
            dma((2,)),
            dma((2,)),
            dma((seqs, chips)),
            dma((seqs, chips)),
            dma((seqs, chips, sections - 1)),
            dma((seqs, chips, sections - 1)),
            dma((seqs, chips - 1)),
            dma((seqs, chips - 1)),
            dma((tensors - 1,)),
            dma((tensors - 1,)),
            dma((seqs, tensors - 1)),
            dma((seqs, tensors - 1)),
        ],
        compiler_params=pltpu.CompilerParams(
            collective_id=0, has_side_effects=True, vmem_limit_bytes=60 * 1024 * 1024
        ),
    )
    return call(
        dec_queries, enc_keys, enc_values, out_grad, key_weight, value_weight,
        enc_hidden, enc_gain.reshape(1, feats),
    )


def solution(mesh):
    wide = P("section", "dp", None, "tensor")
    return jax.shard_map(
        functools.partial(per_device, mesh.shape["section"], mesh.shape["tensor"]),
        mesh=mesh,
        in_specs=(
            wide, wide, wide, wide,
            P("section", None, "tensor"),
            P("section", None, "tensor"),
            P("dp", "section", "tensor"),
            P("tensor"),
        ),
        out_specs=P("dp", "section", "tensor"),
        check_vma=False,
    )
```
